32 devices in a mesh: row: 4 (over y, core), col: 8 (over z, x).
Axes of the slice: x: 2, y: 2, z: 4, core: 2. Of those that a mesh axis runs over, the one named last changes fastest.
Arguments:
- excitons: float32 [1024, 1024], P('row', 'col'), may hold values from -500 to 500
- valence_energy: float32 [1024], P('row'), may hold values from -3 to -1
- conduction_energy: float32 [1024], P('col'), may hold values from 1 to 3
- psi_valence: float32 [4096, 1024], P('row', 'col'), may hold values from -0.1875 to 0.1875
- psi_conduction: float32 [4096, 1024], P('col', 'row'), may hold values from -0.1875 to 0.1875
- screened: float32 [4096, 4096], P('row', 'col'), may hold values from -0.9 to 0.975, as said below
Outputs:
- next_vector: float32 [1024, 1024], P('row', 'col')
- coefficients: float32 [4], replicated
The draws below stay inside these ranges and needn't reach their ends.
Inputs may be any that keep to these rules, and one draw needn't show every extreme that they name: symmetric: screened[p, p'] = screened[p', p].
All inputs are finite; a program needn't handle non-finite values.
Results may differ from the reference program's by a relative error of at most 0.0003.
Values sent between devices are 32-bit elements; how exact they have to be, the bound alone decides.
A program may use at most 64 MiB of HBM per device.

```python
import math
import jax
import jax.numpy as jnp
from jax import lax

NV = 1024
NC = 1024
NP = 4096
STEPS = 2


def draw_excitons(key, part):
    base_key = jax.random.fold_in(key, 11)
    key_entries, key_rows, key_cols = jax.random.split(base_key, 3)
    row_scale = 3.0 ** (jnp.arange(NV, dtype=jnp.float32) / NV) * jnp.exp(jax.random.uniform(key_rows, (NV,), jnp.float32, 0.0, math.log(3.2)))
    col_scale = 3.0 ** (jnp.arange(NC, dtype=jnp.float32) / NC) * jnp.exp(jax.random.uniform(key_cols, (NC,), jnp.float32, 0.0, math.log(3.2)))
    entries = jnp.clip(jax.random.normal(key_entries, (NV, NC), jnp.float32), -5.0, 5.0)
    return (entries * row_scale[:, None] * col_scale[None, :]).astype(jnp.float32)


def draw_screened(key, part):
    base_key = jax.random.fold_in(key, 23)
    noise_scale = 0.6 * (NV * NC) ** 0.5 / NP
    smooth_height = 1.2 * NV * NC / (NP * NP)
    places = jnp.arange(NP, dtype=jnp.float32)
    distance = jnp.abs(places[:, None] - places[None, :])
    noise = jnp.clip(jax.random.normal(base_key, (NP, NP), jnp.float32), -4.0, 4.0)
    reach = NP / 8.0
    symmetric = (noise + noise.T) * (1.0 / math.sqrt(2.0))
    smooth = smooth_height * jnp.exp(-distance / reach)
    return (noise_scale * symmetric + smooth).astype(jnp.float32)


def levels(own_key, shape, pieces, smallest, largest):
    level = 1.0
    for axis_at, parts in pieces:
        steps = jax.random.uniform(jax.random.fold_in(jax.random.fold_in(own_key, 6), axis_at), (parts,), jnp.float32, smallest / len(pieces), largest / len(pieces))
        level = level * jnp.repeat(jnp.exp(steps), shape[axis_at] // parts).reshape((-1,) + (1,) * (len(shape) - 1 - axis_at))
    return level


def normal_values(stream_key, shape, deviation, limit, shards=(), kind=jnp.bfloat16):
    array = jax.random.normal(stream_key, shape, jnp.float32) * deviation
    if len(shards) > 0:
        array = levels(stream_key, shape, shards, -0.22, 0.18) * array
    return jnp.clip(array, min=-limit, max=limit).astype(kind)


def setup_inputs(seed: int = 0) -> dict:
    seeds = jax.random.split(jax.random.key(seed), 7)
    return {
        "excitons": draw_excitons(jax.random.fold_in(seeds[6], 71), 0),
        "valence_energy": jnp.clip(-3.0 + 2.0 * jax.random.uniform(seeds[1], (NV,), jnp.float32) ** levels(seeds[1], (NV,), ((0, 4),), -0.2, 0.2), -3.0, -1.0),
        "conduction_energy": jnp.clip(1.0 + 2.0 * jax.random.uniform(seeds[2], (NC,), jnp.float32) ** levels(seeds[2], (NC,), ((0, 8),), -0.2, 0.2), 1.0, 3.0),
        "psi_valence": normal_values(seeds[3], (NP, NV), NV ** -0.5, 0.1875, ((0, 4), (1, 8)), jnp.float32),
        "psi_conduction": normal_values(seeds[4], (NP, NC), NC ** -0.5, 0.1875, ((0, 8), (1, 4)), jnp.float32),
        "screened": draw_screened(jax.random.fold_in(seeds[6], 71), 0),
    }


EPS = 1e-06

def inner(left, right):
    return jnp.sum(left * right) / (NV * NC)

def apply_operator(vector, valence_energy, conduction_energy, psi_valence, psi_conduction, screened):
    high = lax.Precision.HIGHEST
    image = jnp.dot(vector, psi_conduction.T, precision=high)
    points = jnp.dot(psi_valence, image, precision=high)
    weighted = points * screened
    back_valence = jnp.dot(psi_valence.T, weighted, precision=high)
    kernel = jnp.dot(back_valence, psi_conduction, precision=high)
    energy_gap = conduction_energy[None, :] - valence_energy[:, None]
    return energy_gap * vector - kernel

def reference(excitons, valence_energy, conduction_energy, psi_valence, psi_conduction, screened):
    vector = excitons / jnp.sqrt(inner(excitons, excitons) + EPS)
    previous = jnp.zeros_like(vector)
    beta_prev = jnp.zeros((), jnp.float32)
    values = []
    for step in range(STEPS):
        image = apply_operator(vector, valence_energy, conduction_energy, psi_valence, psi_conduction, screened)
        alpha = inner(vector, image)
        residual = image - alpha * vector - beta_prev * previous
        beta = jnp.sqrt(inner(residual, residual) + EPS)
        previous = vector
        vector = residual / beta
        beta_prev = beta
        values.append(alpha)
        values.append(beta)
    return (vector, jnp.stack(values))
```

```python
import jax
import jax.numpy as jnp
from jax import lax
from jax.experimental import pallas as pl
from jax.experimental.pallas import tpu as pltpu
from jax.sharding import PartitionSpec as P

NV = 1024
NC = 1024
STEPS = 2


EPS = 1e-06


def shards(excitons, valence_energy, conduction_energy, psi_valence, psi_conduction, screened):
    high = lax.Precision.HIGHEST
    count = NV * NC
    energy_gap = conduction_energy[None, :] - valence_energy[:, None]
    total = lax.psum(jnp.sum(excitons * excitons), ("row", "col"))
    vector = excitons / jnp.sqrt(total / count + EPS)
    previous = jnp.zeros_like(vector)
    beta_prev = jnp.zeros((), jnp.float32)
    values = []
    for step in range(STEPS):
        panel_valence = lax.all_gather(psi_valence, "col", axis=1, tiled=True)
        panel_conduction = lax.all_gather(psi_conduction, "row", axis=1, tiled=True)
        full_rows = lax.all_gather(vector, "col", axis=1, tiled=True)
        image_block = jnp.dot(full_rows, panel_conduction.T, precision=high)
        image_columns = lax.all_gather(image_block, "row", axis=0, tiled=True)
        points = jnp.dot(panel_valence, image_columns, precision=high)
        weighted = points * screened
        back_valence = lax.psum_scatter(
            jnp.dot(panel_valence.T, weighted, precision=high),
            "row",
            scatter_dimension=0,
            tiled=True,
        )
        back_flipped = back_valence.T
        kernel_flipped = lax.psum_scatter(
            jnp.dot(panel_conduction.T, back_flipped, precision=high),
            "col",
            scatter_dimension=0,
            tiled=True,
        )
        image = energy_gap * vector - kernel_flipped.T
        cross, square, older = lax.psum(
            (jnp.sum(vector * image), jnp.sum(image * image), jnp.sum(previous * image)),
            ("row", "col"),
        )
        alpha = cross / count
        residual = image - alpha * vector - beta_prev * previous
        squared = (
            square / count - alpha * alpha - 2.0 * beta_prev * older / count + beta_prev * beta_prev
        )
        beta = jnp.sqrt(squared + EPS)
        previous = vector
        vector = residual / beta
        beta_prev = beta
        values.append(alpha)
        values.append(beta)
    return (vector, jnp.stack(values))


MESH = pl.DeviceIdType.MESH
NN = (((1,), (0,)), ((), ()))
NT = (((1,), (1,)), ((), ()))


def halves(value):
    hi = value.astype(jnp.bfloat16)
    return hi, (value - hi.astype(jnp.float32)).astype(jnp.bfloat16)


def dot3(a, b, dims):
    dot = lambda u, v: lax.dot_general(u, v, dims, preferred_element_type=jnp.float32)
    return dot(a[0], b[0]) + (dot(a[0], b[1]) + dot(a[1], b[0]))


def fused(
    R, C, count,
    x_ref, ve_ref, ce_ref, pv_ref, pc_ref, w_ref,
    out_ref, coef_ref,
    xl, pvl, pcl, il, cr, yr, xr, zr, bk, kb, sa, sb,
    pv3, pc3, xs, im, wt, acc, wtr, q1, gap,
    qz_s, qz_r, qx_s, qx_r, vz_s, vz_r, vx_s, vx_r,
    cy_s, cy_r, cc_s, cc_r, iy_s, iy_r, ic_s, ic_r,
    cr_s, cr_r, yr_s, yr_r, xr_s, xr_r, zr_s, zr_r,
    sa_s, sa_r, sb_s, sb_r,
):
    NY, NZ = R // 2, C // 2
    r, c = lax.axis_index("row"), lax.axis_index("col")
    y, k, z, h = r // 2, r % 2, c // 2, c % 2
    pending = []

    def copy(src, dst, ss, rs, dev):
        return pltpu.make_async_remote_copy(
            src_ref=src, dst_ref=dst, send_sem=ss, recv_sem=rs, device_id=dev, device_id_type=MESH
        )

    def send(src, dst, ss, rs, dev):
        op = copy(src, dst, ss, rs, dev)
        op.start()
        pending.append(op)

    def wait(dst, ss, rs):
        copy(dst, dst, ss, rs, (r, c)).wait_recv()

    zdev = lambda d: (r, ((z + d) % NZ) * 2 + h)
    zsrc = lambda d: ((z - d + NZ) % NZ) * 2 + h
    xpeer = (r, z * 2 + 1 - h)
    ydev = lambda d: (((y + d) % NY) * 2 + k, c)
    ysrc = lambda d: ((y - d + NY) % NY) * 2 + k
    kpeer = (y * 2 + 1 - k, c)
    near = [d for d in range(1, NZ) if d in (1, NZ - 1)] + [d for d in range(2, NZ - 1)]

    barrier = pltpu.get_barrier_semaphore()
    for d in range(1, C):
        pl.semaphore_signal(barrier, inc=1, device_id=(r, (c + d) % C), device_id_type=MESH)
    for d in range(1, R):
        pl.semaphore_signal(barrier, inc=1, device_id=((r + d) % R, c), device_id_type=MESH)
    pl.semaphore_wait(barrier, C + R - 2)

    def col_z(own, land, ss, rs):
        for d in near:
            send(own, land.at[c], ss.at[d], rs.at[d], zdev(d))

    def col_own(own, land, ss, rs):
        send(own, land.at[c], ss.at[0], rs.at[0], xpeer)

    def col_forward(d, land, zs, zr_, ss, rs):
        slot = land.at[zsrc(d)]
        wait(slot, zs.at[d], zr_.at[d])
        send(slot, slot, ss.at[d], rs.at[d], xpeer)

    def col_done(d, land, ss, rs):
        wait(land.at[((z - d + NZ) % NZ) * 2 + 1 - h], ss.at[d], rs.at[d])

    def row_start(own, land, ys, yr_, cs, cr_):
        for d in range(1, NY):
            send(own, land.at[r], ys.at[d], yr_.at[d], ydev(d))
        send(own, land.at[r], cs.at[0], cr_.at[0], kpeer)

    def row_forward(d, land, ys, yr_, cs, cr_):
        slot = land.at[ysrc(d)]
        wait(slot, ys.at[d], yr_.at[d])
        send(slot, slot, cs.at[d], cr_.at[d], kpeer)

    def row_done(d, land, cs, cr_):
        wait(land.at[((y - d + NY) % NY) * 2 + 1 - k], cs.at[d], cr_.at[d])

    def reduce_start(i, values):
        rows = [jnp.broadcast_to(v.reshape(1, 1), (1, 128)) for v in values]
        rows += [jnp.zeros((1, 128), jnp.float32)] * (8 - len(rows))
        sa[i, c] = jnp.concatenate(rows, axis=0)
        for d in range(1, C):
            send(sa.at[i, c], sa.at[i, c], sa_s.at[i, d], sa_r.at[i, d], (r, (c + d) % C))

    def reduce_middle(i):
        for d in range(1, C):
            wait(sa.at[i, (c - d + C) % C], sa_s.at[i, d], sa_r.at[i, d])
        sb[i, r] = jnp.sum(sa[i], axis=0)
        for d in range(1, R):
            send(sb.at[i, r], sb.at[i, r], sb_s.at[i, d], sb_r.at[i, d], ((r + d) % R, c))

    def reduce_end(i):
        for d in range(1, R):
            wait(sb.at[i, (r - d + R) % R], sb_s.at[i, d], sb_r.at[i, d])
        total = jnp.sum(sb[i], axis=0)
        return [total[j : j + 1, :] for j in range(3)]

    col_z(x_ref, xl.at[0], qz_s.at[0], qz_r.at[0])
    col_own(x_ref, xl.at[0], qx_s.at[0], qx_r.at[0])
    row_start(pc_ref, pcl, cy_s, cy_r, cc_s, cc_r)
    col_z(pv_ref, pvl, vz_s, vz_r)
    start = x_ref[...]
    xl[0, c] = start
    reduce_start(0, [jnp.sum(start * start)])
    for d in near:
        col_forward(d, xl.at[0], qz_s.at[0], qz_r.at[0], qx_s.at[0], qx_r.at[0])
    col_own(pv_ref, pvl, vx_s, vx_r)
    reduce_middle(0)
    wtr[...] = w_ref[...].T
    ve = jnp.broadcast_to(ve_ref[...], (ce_ref.shape[1], ve_ref.shape[1])).T
    gap[...] = ce_ref[...] - ve
    for d in range(1, NY):
        row_forward(d, pcl, cy_s, cy_r, cc_s, cc_r)
    ncl = x_ref.shape[1]

    def split_pv(b, half):
        hi, lo = halves(pvl[b] if half is None else half)
        return hi, lo

    def put_pv(block_z, block_h, value):
        hi, lo = halves(value)
        col = pl.ds(pl.multiple_of(block_h * ncl, 128), ncl)
        pv3[0, block_z, :, col] = hi
        pv3[1, block_z, :, col] = lo

    def put_pc(block, value):
        hi, lo = halves(value)
        pc3[0, block] = hi
        pc3[1, block] = lo

    put_pc(r, pc_ref[...])
    put_pv(z, h, pv_ref[...])
    for d in range(NY):
        row_done(d, pcl, cc_s, cc_r)
    for d in range(1, R):
        other = (r + d) % R
        put_pc(other, pcl[other])
    (total,) = reduce_end(0)[:1]
    scale = 1.0 / jnp.sqrt(total / count + EPS)
    q1[...] = start * scale
    for d in range(NZ):
        col_done(d, xl.at[0], qx_s.at[0], qx_r.at[0])

    tile = 128
    points = pc_ref.shape[0]
    betas = None
    for s in range(2):
        for zz in range(NZ):
            for hh in range(2):
                b = zz * 2 + hh
                if s == 0:
                    value = xl[0, b] * scale
                else:
                    value = (xl[1, b] - alpha * (xl[0, b] * scale)) / beta
                hi, lo = halves(value)
                xs[0, zz, :, hh * ncl : (hh + 1) * ncl] = hi
                xs[1, zz, :, hh * ncl : (hh + 1) * ncl] = lo
        total = None
        for zz in range(NZ):
            part = dot3((pc3[0, zz], pc3[1, zz]), (xs[0, zz], xs[1, zz]), NT)
            total = part if total is None else total + part
        il[s, r] = total
        row_start(il.at[s, r], il.at[s], iy_s.at[s], iy_r.at[s], ic_s.at[s], ic_r.at[s])
        if s == 0:
            for d in near:
                col_forward(d, pvl, vz_s, vz_r, vx_s, vx_r)
                put_pv((z - d + NZ) % NZ, h, pvl[zsrc(d)])
                if d == near[0]:
                    for e in range(1, NY):
                        row_forward(e, il.at[s], iy_s.at[s], iy_r.at[s], ic_s.at[s], ic_r.at[s])
            for d in [0] + near:
                col_done(d, pvl, vx_s, vx_r)
                zz = (z - d + NZ) % NZ
                put_pv(zz, 1 - h, pvl[zz * 2 + 1 - h])

        def chunk(b, first):
            im[0], im[1] = halves(il[s, b])

            def body(i, carry):
                rows = pl.ds(pl.multiple_of(i * tile, tile), tile)
                part = dot3((im[0, rows], im[1, rows]), (pv3[0, b], pv3[1, b]), NT)
                acc[rows, :] = part if first else acc[rows, :] + part
                return carry

            lax.fori_loop(0, points // tile, body, 0)

        chunk(r, True)
        row_done(0, il.at[s], ic_s.at[s], ic_r.at[s])
        chunk(y * 2 + 1 - k, False)
        for e in range(1, NY):
            if s == 1:
                row_forward(e, il.at[s], iy_s.at[s], iy_r.at[s], ic_s.at[s], ic_r.at[s])
            chunk(ysrc(e), False)
            row_done(e, il.at[s], ic_s.at[s], ic_r.at[s])
            chunk(((y - e + NY) % NY) * 2 + 1 - k, False)
        wt[0], wt[1] = halves(acc[...] * wtr[...])

        def back(b):
            def body(i, carry):
                rows = pl.ds(pl.multiple_of(i * tile, tile), tile)
                bk[s, b, rows, :] = dot3((wt[0, rows], wt[1, rows]), (pv3[0, b], pv3[1, b]), NN)
                return carry

            lax.fori_loop(0, points // tile, body, 0)

        for d in [*range(1, NY), 0]:
            mine, theirs = ((y + d) % NY) * 2 + k, ((y + d) % NY) * 2 + 1 - k
            back(theirs)
            send(bk.at[s, theirs], cr.at[s, d], cr_s.at[s, d], cr_r.at[s, d], kpeer)
            back(mine)
            wait(cr.at[s, d], cr_s.at[s, d], cr_r.at[s, d])
            bk[s, mine] = bk[s, mine] + cr[s, d]
            if d > 0:
                send(bk.at[s, mine], yr.at[s, d], yr_s.at[s, d], yr_r.at[s, d], ydev(d))
        summed = bk[s, r]
        for d in range(1, NY):
            wait(yr.at[s, d], yr_s.at[s, d], yr_r.at[s, d])
            summed = summed + yr[s, d]
        flat = halves(summed.T)
        far = [d for d in range(2, NZ - 1)] + [d for d in range(1, NZ) if d in (1, NZ - 1)] + [0]
        for d in far:
            zz = (z + d) % NZ
            part = dot3(flat, (pc3[0, zz], pc3[1, zz]), NN)
            kb[s, d, 0] = part[:, :ncl]
            kb[s, d, 1] = part[:, ncl:]
            send(kb.at[s, d, 1 - h], xr.at[s, d], xr_s.at[s, d], xr_r.at[s, d], xpeer)
        for d in far:
            wait(xr.at[s, d], xr_s.at[s, d], xr_r.at[s, d])
            kb[s, d, h] = kb[s, d, h] + xr[s, d]
            if d > 0:
                send(kb.at[s, d, h], zr.at[s, d], zr_s.at[s, d], zr_r.at[s, d], zdev(d))
        kernel = kb[s, 0, h]
        for d in near:
            wait(zr.at[s, d], zr_s.at[s, d], zr_r.at[s, d])
            kernel = kernel + zr[s, d]
        if s == 0:
            vector = q1[...]
            image = gap[...] * vector - kernel
            xl[1, c] = image
            col_z(xl.at[1, c], xl.at[1], qz_s.at[1], qz_r.at[1])
            col_own(xl.at[1, c], xl.at[1], qx_s.at[1], qx_r.at[1])
            reduce_start(1, [jnp.sum(vector * image), jnp.sum(image * image)])
            reduce_middle(1)
            for d in near:
                col_forward(d, xl.at[1], qz_s.at[1], qz_r.at[1], qx_s.at[1], qx_r.at[1])
            cross, square, _ = reduce_end(1)
            alpha = cross / count
            beta = jnp.sqrt(square / count - alpha * alpha + EPS)
            coef_ref[0:1, :] = alpha
            coef_ref[1:2, :] = beta
            for d in range(NZ):
                col_done(d, xl.at[1], qx_s.at[1], qx_r.at[1])
        else:
            vector = (xl[1, c] - alpha * q1[...]) / beta
            previous = q1[...]
            image = gap[...] * vector - kernel
            reduce_start(2, [jnp.sum(vector * image), jnp.sum(image * image), jnp.sum(previous * image)])
            reduce_middle(2)
            cross, square, older = reduce_end(2)
            alpha2 = cross / count
            squared = square / count - alpha2 * alpha2 - 2.0 * beta * older / count + beta * beta
            beta2 = jnp.sqrt(squared + EPS)
            out_ref[...] = (image - alpha2 * vector - beta * previous) / beta2
            coef_ref[2:3, :] = alpha2
            coef_ref[3:4, :] = beta2
    for op in pending:
        op.wait_send()


def fused_shards(R, C, excitons, valence_energy, conduction_energy, psi_valence, psi_conduction, screened):
    nv, nc = excitons.shape
    pr, pcn = screened.shape
    f32, bf16 = jnp.float32, jnp.bfloat16
    NY, NZ = R // 2, C // 2
    vm, dma = pltpu.VMEM, pltpu.SemaphoreType.DMA
    count = float(NV * NC)
    scratch = [
        vm((2, C, nv, nc), f32), vm((C, pr, nc), f32), vm((R, pcn, nv), f32), vm((2, R, pcn, nv), f32),
        vm((2, NY, pcn, nv), f32), vm((2, NY, pcn, nv), f32),
        vm((2, NZ, nv, nc), f32), vm((2, NZ, nv, nc), f32),
        vm((2, R, pcn, nv), f32), vm((2, NZ, 2, nv, nc), f32),
        vm((3, C, 8, 128), f32), vm((3, R, 8, 128), f32),
        vm((2, R, pr, nv), bf16), vm((2, NZ, pcn, 2 * nc), bf16), vm((2, NZ, nv, 2 * nc), bf16),
        vm((2, pcn, nv), bf16), vm((2, pcn, pr), bf16), vm((pcn, pr), f32), vm((pcn, pr), f32),
        vm((nv, nc), f32), vm((nv, nc), f32),
    ]
    pairs = [(2, NZ), (2, NZ), (NZ,), (NZ,), (NY,), (NY,), (2, NY), (2, NY), (2, NY), (2, NY), (2, NZ), (2, NZ), (3, C), (3, R)]
    for shape in pairs:
        scratch += [dma(shape), dma(shape)]
    vector, coef = pl.pallas_call(
        lambda *refs: fused(R, C, count, *refs),
        out_shape=(jax.ShapeDtypeStruct((nv, nc), f32), jax.ShapeDtypeStruct((4, 128), f32)),
        in_specs=[pl.BlockSpec(memory_space=vm)] * 6,
        out_specs=(pl.BlockSpec(memory_space=vm), pl.BlockSpec(memory_space=vm)),
        scratch_shapes=scratch,
        compiler_params=pltpu.CompilerParams(collective_id=0, has_side_effects=True, vmem_limit_bytes=67043328),
    )(excitons, valence_energy.reshape(1, nv), conduction_energy.reshape(1, nc), psi_valence, psi_conduction, screened)
    return vector, coef[:, 0]


def solution(mesh):
    R, C = mesh.shape["row"], mesh.shape["col"]
    aligned = C == 2 * R and R % 2 == 0 and STEPS == 2 and NV == NC and (NV // R) % 128 == 0 and (NC // C) % 128 == 0
    body = (lambda *args: fused_shards(R, C, *args)) if aligned else shards
    return jax.shard_map(
        body,
        mesh=mesh,
        in_specs=(
            P("row", "col"),
            P("row"),
            P("col"),
            P("row", "col"),
            P("col", "row"),
            P("row", "col"),
        ),
        out_specs=(P("row", "col"), P()),
        check_vma=False,
    )
```

```python
import jax
import jax.numpy as jnp
from jax import lax
from jax.experimental import pallas as pl
from jax.experimental.pallas import tpu as pltpu
from jax.sharding import PartitionSpec as P

NV = 1024
NC = 1024
STEPS = 2


EPS = 1e-06


def shards(excitons, valence_energy, conduction_energy, psi_valence, psi_conduction, screened):
    high = lax.Precision.HIGHEST
    count = NV * NC
    energy_gap = conduction_energy[None, :] - valence_energy[:, None]
    total = lax.psum(jnp.sum(excitons * excitons), ("row", "col"))
    vector = excitons / jnp.sqrt(total / count + EPS)
    previous = jnp.zeros_like(vector)
    beta_prev = jnp.zeros((), jnp.float32)
    values = []
    for step in range(STEPS):
        panel_valence = lax.all_gather(psi_valence, "col", axis=1, tiled=True)
        panel_conduction = lax.all_gather(psi_conduction, "row", axis=1, tiled=True)
        full_rows = lax.all_gather(vector, "col", axis=1, tiled=True)
        image_block = jnp.dot(full_rows, panel_conduction.T, precision=high)
        image_columns = lax.all_gather(image_block, "row", axis=0, tiled=True)
        points = jnp.dot(panel_valence, image_columns, precision=high)
        weighted = points * screened
        back_valence = lax.psum_scatter(
            jnp.dot(panel_valence.T, weighted, precision=high),
            "row",
            scatter_dimension=0,
            tiled=True,
        )
        back_flipped = back_valence.T
        kernel_flipped = lax.psum_scatter(
            jnp.dot(panel_conduction.T, back_flipped, precision=high),
            "col",
            scatter_dimension=0,
            tiled=True,
        )
        image = energy_gap * vector - kernel_flipped.T
        cross, square, older = lax.psum(
            (jnp.sum(vector * image), jnp.sum(image * image), jnp.sum(previous * image)),
            ("row", "col"),
        )
        alpha = cross / count
        residual = image - alpha * vector - beta_prev * previous
        squared = (
            square / count - alpha * alpha - 2.0 * beta_prev * older / count + beta_prev * beta_prev
        )
        beta = jnp.sqrt(squared + EPS)
        previous = vector
        vector = residual / beta
        beta_prev = beta
        values.append(alpha)
        values.append(beta)
    return (vector, jnp.stack(values))


MESH = pl.DeviceIdType.MESH
NN = (((1,), (0,)), ((), ()))
NT = (((1,), (1,)), ((), ()))


def halves(value):
    hi = value.astype(jnp.bfloat16)
    return hi, (value - hi.astype(jnp.float32)).astype(jnp.bfloat16)


def dot3(a, b, dims):
    dot = lambda u, v: lax.dot_general(u, v, dims, preferred_element_type=jnp.float32)
    return dot(a[0], b[0]) + (dot(a[0], b[1]) + dot(a[1], b[0]))


def fused(
    R, C, count,
    x_ref, ve_ref, ce_ref, pv_ref, pc_ref, w_ref,
    out_ref, coef_ref,
    xl, pvl, pcl, il, cr, yr, xr, zr, bk, kb, sa, sb,
    pv3, pc3, xs, im, wt, acc, wtr, q1, gap,
    qz_s, qz_r, qx_s, qx_r, vz_s, vz_r, vx_s, vx_r,
    cy_s, cy_r, cc_s, cc_r, iy_s, iy_r, ic_s, ic_r,
    cr_s, cr_r, yr_s, yr_r, xr_s, xr_r, zr_s, zr_r,
    sa_s, sa_r, sb_s, sb_r,
):
    NY, NZ = R // 2, C // 2
    r, c = lax.axis_index("row"), lax.axis_index("col")
    y, k, z, h = r // 2, r % 2, c // 2, c % 2
    pending = []

    def copy(src, dst, ss, rs, dev):
        return pltpu.make_async_remote_copy(
            src_ref=src, dst_ref=dst, send_sem=ss, recv_sem=rs, device_id=dev, device_id_type=MESH
        )

    def send(src, dst, ss, rs, dev):
        op = copy(src, dst, ss, rs, dev)
        op.start()
        pending.append(op)

    def wait(dst, ss, rs):
        copy(dst, dst, ss, rs, (r, c)).wait_recv()

    zdev = lambda d: (r, ((z + d) % NZ) * 2 + h)
    zsrc = lambda d: ((z - d + NZ) % NZ) * 2 + h
    xpeer = (r, z * 2 + 1 - h)
    ydev = lambda d: (((y + d) % NY) * 2 + k, c)
    ysrc = lambda d: ((y - d + NY) % NY) * 2 + k
    kpeer = (y * 2 + 1 - k, c)
    near = [d for d in range(1, NZ) if d in (1, NZ - 1)] + [d for d in range(2, NZ - 1)]

    barrier = pltpu.get_barrier_semaphore()
    for d in range(1, C):
        pl.semaphore_signal(barrier, inc=1, device_id=(r, (c + d) % C), device_id_type=MESH)
    for d in range(1, R):
        pl.semaphore_signal(barrier, inc=1, device_id=((r + d) % R, c), device_id_type=MESH)
    pl.semaphore_wait(barrier, C + R - 2)

    def col_z(own, land, ss, rs):
        for d in near:
            send(own, land.at[c], ss.at[d], rs.at[d], zdev(d))

    def col_own(own, land, ss, rs):
        send(own, land.at[c], ss.at[0], rs.at[0], xpeer)

    def col_forward(d, land, zs, zr_, ss, rs):
        slot = land.at[zsrc(d)]
        wait(slot, zs.at[d], zr_.at[d])
        send(slot, slot, ss.at[d], rs.at[d], xpeer)

    def col_done(d, land, ss, rs):
        wait(land.at[((z - d + NZ) % NZ) * 2 + 1 - h], ss.at[d], rs.at[d])

    def row_start(own, land, ys, yr_, cs, cr_):
        for d in range(1, NY):
            send(own, land.at[r], ys.at[d], yr_.at[d], ydev(d))
        send(own, land.at[r], cs.at[0], cr_.at[0], kpeer)

    def row_forward(d, land, ys, yr_, cs, cr_):
        slot = land.at[ysrc(d)]
        wait(slot, ys.at[d], yr_.at[d])
        send(slot, slot, cs.at[d], cr_.at[d], kpeer)

    def row_done(d, land, cs, cr_):
        wait(land.at[((y - d + NY) % NY) * 2 + 1 - k], cs.at[d], cr_.at[d])

    def reduce_start(i, values):
        rows = [jnp.broadcast_to(v.reshape(1, 1), (1, 128)) for v in values]
        rows += [jnp.zeros((1, 128), jnp.float32)] * (8 - len(rows))
        sa[i, c] = jnp.concatenate(rows, axis=0)
        for d in range(1, C):
            send(sa.at[i, c], sa.at[i, c], sa_s.at[i, d], sa_r.at[i, d], (r, (c + d) % C))

    def reduce_middle(i):
        for d in range(1, C):
            wait(sa.at[i, (c - d + C) % C], sa_s.at[i, d], sa_r.at[i, d])
        sb[i, r] = jnp.sum(sa[i], axis=0)
        for d in range(1, R):
            send(sb.at[i, r], sb.at[i, r], sb_s.at[i, d], sb_r.at[i, d], ((r + d) % R, c))

    def reduce_end(i):
        for d in range(1, R):
            wait(sb.at[i, (r - d + R) % R], sb_s.at[i, d], sb_r.at[i, d])
        total = jnp.sum(sb[i], axis=0)
        return [total[j : j + 1, :] for j in range(3)]

    col_z(x_ref, xl.at[0], qz_s.at[0], qz_r.at[0])
    col_own(x_ref, xl.at[0], qx_s.at[0], qx_r.at[0])
    row_start(pc_ref, pcl, cy_s, cy_r, cc_s, cc_r)
    half = pv_ref.shape[0] // 2
    part_of = lambda j: pl.ds(j * half, half)
    for j in range(2):
        col_z(pv_ref.at[part_of(j)], pvl.at[j], vz_s.at[j], vz_r.at[j])
    start = x_ref[...]
    xl[0, c] = start
    reduce_start(0, [jnp.sum(start * start)])
    for d in near:
        col_forward(d, xl.at[0], qz_s.at[0], qz_r.at[0], qx_s.at[0], qx_r.at[0])
    for j in range(2):
        col_own(pv_ref.at[part_of(j)], pvl.at[j], vx_s.at[j], vx_r.at[j])
    reduce_middle(0)
    wtr[...] = w_ref[...].T
    ve = jnp.broadcast_to(ve_ref[...], (ce_ref.shape[1], ve_ref.shape[1])).T
    gap[...] = ce_ref[...] - ve
    for d in range(1, NY):
        row_forward(d, pcl, cy_s, cy_r, cc_s, cc_r)
    ncl = x_ref.shape[1]

    def put_pv(j, block_z, block_h, value):
        hi, lo = halves(value)
        col = pl.ds(pl.multiple_of(block_h * ncl, 128), ncl)
        pv3[0, block_z, part_of(j), col] = hi
        pv3[1, block_z, part_of(j), col] = lo

    def put_pc(block, value):
        hi, lo = halves(value)
        pc3[0, block] = hi
        pc3[1, block] = lo

    put_pc(r, pc_ref[...])
    for j in range(2):
        put_pv(j, z, h, pv_ref[part_of(j), :])
    for d in range(NY):
        row_done(d, pcl, cc_s, cc_r)
    for d in range(1, R):
        other = (r + d) % R
        put_pc(other, pcl[other])
    (total,) = reduce_end(0)[:1]
    scale = 1.0 / jnp.sqrt(total / count + EPS)
    q1[...] = start * scale
    for d in range(NZ):
        col_done(d, xl.at[0], qx_s.at[0], qx_r.at[0])

    points = pc_ref.shape[0]
    tile = points // 2
    betas = None
    for s in range(2):
        for zz in range(NZ):
            for hh in range(2):
                b = zz * 2 + hh
                if s == 0:
                    value = xl[0, b] * scale
                else:
                    value = (xl[1, b] - alpha * (xl[0, b] * scale)) / beta
                hi, lo = halves(value)
                xs[0, zz, :, hh * ncl : (hh + 1) * ncl] = hi
                xs[1, zz, :, hh * ncl : (hh + 1) * ncl] = lo
        total = None
        for zz in range(NZ):
            part = dot3((pc3[0, zz], pc3[1, zz]), (xs[0, zz], xs[1, zz]), NT)
            total = part if total is None else total + part
        il[s, r] = total
        row_start(il.at[s, r], il.at[s], iy_s.at[s], iy_r.at[s], ic_s.at[s], ic_r.at[s])
        if s == 0:
            for d in near:
                for j in range(2):
                    col_forward(d, pvl.at[j], vz_s.at[j], vz_r.at[j], vx_s.at[j], vx_r.at[j])
                    put_pv(j, (z - d + NZ) % NZ, h, pvl[j, zsrc(d)])
                if d == near[0]:
                    for e in range(1, NY):
                        row_forward(e, il.at[s], iy_s.at[s], iy_r.at[s], ic_s.at[s], ic_r.at[s])
            for d in [0] + near:
                for j in range(2):
                    col_done(d, pvl.at[j], vx_s.at[j], vx_r.at[j])
                    zz = (z - d + NZ) % NZ
                    put_pv(j, zz, 1 - h, pvl[j, zz * 2 + 1 - h])

        def chunk(b, first):
            im[0], im[1] = halves(il[s, b])

            def body(i, carry):
                rows = pl.ds(pl.multiple_of(i * tile, tile), tile)
                part = dot3((im[0, rows], im[1, rows]), (pv3[0, b], pv3[1, b]), NT)
                acc[rows, :] = part if first else acc[rows, :] + part
                return carry

            lax.fori_loop(0, points // tile, body, 0)

        chunk(r, True)
        row_done(0, il.at[s], ic_s.at[s], ic_r.at[s])
        chunk(y * 2 + 1 - k, False)
        for e in range(1, NY):
            if s == 1:
                row_forward(e, il.at[s], iy_s.at[s], iy_r.at[s], ic_s.at[s], ic_r.at[s])
            chunk(ysrc(e), False)
            row_done(e, il.at[s], ic_s.at[s], ic_r.at[s])
            chunk(((y - e + NY) % NY) * 2 + 1 - k, False)
        wt[0], wt[1] = halves(acc[...] * wtr[...])

        def back(b):
            def body(i, carry):
                rows = pl.ds(pl.multiple_of(i * tile, tile), tile)
                bk[s, b, rows, :] = dot3((wt[0, rows], wt[1, rows]), (pv3[0, b], pv3[1, b]), NN)
                return carry

            lax.fori_loop(0, points // tile, body, 0)

        for d in [*range(1, NY), 0]:
            mine, theirs = ((y + d) % NY) * 2 + k, ((y + d) % NY) * 2 + 1 - k
            back(theirs)
            send(bk.at[s, theirs], cr.at[s, d], cr_s.at[s, d], cr_r.at[s, d], kpeer)
            back(mine)
            wait(cr.at[s, d], cr_s.at[s, d], cr_r.at[s, d])
            bk[s, mine] = bk[s, mine] + cr[s, d]
            if d > 0:
                send(bk.at[s, mine], yr.at[s, d], yr_s.at[s, d], yr_r.at[s, d], ydev(d))
        summed = bk[s, r]
        for d in range(1, NY):
            wait(yr.at[s, d], yr_s.at[s, d], yr_r.at[s, d])
            summed = summed + yr[s, d]
        flat = halves(summed.T)
        far = [d for d in range(2, NZ - 1)] + [d for d in range(1, NZ) if d in (1, NZ - 1)] + [0]
        for d in far:
            zz = (z + d) % NZ
            part = dot3(flat, (pc3[0, zz], pc3[1, zz]), NN)
            kb[s, d, 0] = part[:, :ncl]
            kb[s, d, 1] = part[:, ncl:]
            send(kb.at[s, d, 1 - h], xr.at[s, d], xr_s.at[s, d], xr_r.at[s, d], xpeer)
        for d in far:
            wait(xr.at[s, d], xr_s.at[s, d], xr_r.at[s, d])
            kb[s, d, h] = kb[s, d, h] + xr[s, d]
            if d > 0:
                send(kb.at[s, d, h], zr.at[s, d], zr_s.at[s, d], zr_r.at[s, d], zdev(d))
        kernel = kb[s, 0, h]
        for d in near:
            wait(zr.at[s, d], zr_s.at[s, d], zr_r.at[s, d])
            kernel = kernel + zr[s, d]
        if s == 0:
            vector = q1[...]
            image = gap[...] * vector - kernel
            xl[1, c] = image
            col_z(xl.at[1, c], xl.at[1], qz_s.at[1], qz_r.at[1])
            col_own(xl.at[1, c], xl.at[1], qx_s.at[1], qx_r.at[1])
            reduce_start(1, [jnp.sum(vector * image), jnp.sum(image * image)])
            reduce_middle(1)
            for d in near:
                col_forward(d, xl.at[1], qz_s.at[1], qz_r.at[1], qx_s.at[1], qx_r.at[1])
            cross, square, _ = reduce_end(1)
            alpha = cross / count
            beta = jnp.sqrt(square / count - alpha * alpha + EPS)
            coef_ref[0:1, :] = alpha
            coef_ref[1:2, :] = beta
            for d in range(NZ):
                col_done(d, xl.at[1], qx_s.at[1], qx_r.at[1])
        else:
            vector = (xl[1, c] - alpha * q1[...]) / beta
            previous = q1[...]
            image = gap[...] * vector - kernel
            reduce_start(2, [jnp.sum(vector * image), jnp.sum(image * image), jnp.sum(previous * image)])
            reduce_middle(2)
            cross, square, older = reduce_end(2)
            alpha2 = cross / count
            squared = square / count - alpha2 * alpha2 - 2.0 * beta * older / count + beta * beta
            beta2 = jnp.sqrt(squared + EPS)
            out_ref[...] = (image - alpha2 * vector - beta * previous) / beta2
            coef_ref[2:3, :] = alpha2
            coef_ref[3:4, :] = beta2
    for op in pending:
        op.wait_send()


def fused_shards(R, C, excitons, valence_energy, conduction_energy, psi_valence, psi_conduction, screened):
    nv, nc = excitons.shape
    pr, pcn = screened.shape
    f32, bf16 = jnp.float32, jnp.bfloat16
    NY, NZ = R // 2, C // 2
    vm, dma = pltpu.VMEM, pltpu.SemaphoreType.DMA
    count = float(NV * NC)
    scratch = [
        vm((2, C, nv, nc), f32), vm((2, C, pr // 2, nc), f32), vm((R, pcn, nv), f32), vm((2, R, pcn, nv), f32),
        vm((2, NY, pcn, nv), f32), vm((2, NY, pcn, nv), f32),
        vm((2, NZ, nv, nc), f32), vm((2, NZ, nv, nc), f32),
        vm((2, R, pcn, nv), f32), vm((2, NZ, 2, nv, nc), f32),
        vm((3, C, 8, 128), f32), vm((3, R, 8, 128), f32),
        vm((2, R, pr, nv), bf16), vm((2, NZ, pcn, 2 * nc), bf16), vm((2, NZ, nv, 2 * nc), bf16),
        vm((2, pcn, nv), bf16), vm((2, pcn, pr), bf16), vm((pcn, pr), f32), vm((pcn, pr), f32),
        vm((nv, nc), f32), vm((nv, nc), f32),
    ]
    pairs = [(2, NZ), (2, NZ), (2, NZ), (2, NZ), (NY,), (NY,), (2, NY), (2, NY), (2, NY), (2, NY), (2, NZ), (2, NZ), (3, C), (3, R)]
    for shape in pairs:
        scratch += [dma(shape), dma(shape)]
    vector, coef = pl.pallas_call(
        lambda *refs: fused(R, C, count, *refs),
        out_shape=(jax.ShapeDtypeStruct((nv, nc), f32), jax.ShapeDtypeStruct((4, 128), f32)),
        in_specs=[pl.BlockSpec(memory_space=vm)] * 6,
        out_specs=(pl.BlockSpec(memory_space=vm), pl.BlockSpec(memory_space=vm)),
        scratch_shapes=scratch,
        compiler_params=pltpu.CompilerParams(collective_id=0, has_side_effects=True, vmem_limit_bytes=67043328),
    )(excitons, valence_energy.reshape(1, nv), conduction_energy.reshape(1, nc), psi_valence, psi_conduction, screened)
    return vector, coef[:, 0]


def solution(mesh):
    R, C = mesh.shape["row"], mesh.shape["col"]
    aligned = C == 2 * R and R % 2 == 0 and STEPS == 2 and NV == NC and (NV // R) % 128 == 0 and (NC // C) % 128 == 0
    body = (lambda *args: fused_shards(R, C, *args)) if aligned else shards
    return jax.shard_map(
        body,
        mesh=mesh,
        in_specs=(
            P("row", "col"),
            P("row"),
            P("col"),
            P("row", "col"),
            P("col", "row"),
            P("row", "col"),
        ),
        out_specs=(P("row", "col"), P()),
        check_vma=False,
    )
```
